32 devices in a mesh: groups: 2 (over y), tensor: 4 (over z), section: 2 (over x), split: 2 (over core).
Axes of the slice: x: 2, y: 2, z: 4, core: 2. Of those that a mesh axis runs over, the one named last changes fastest.
Arguments:
- teacher_hidden: bfloat16 [1024, 16384], P(('groups', 'section', 'split'), 'tensor'), parts along dimension 0, may hold values from -60 to 60, as said below
- teacher_gain: float32 [16384], P('tensor'), may hold values from 0.1 to 1.9
- proj_weight: bfloat16 [16384, 4096], P(('tensor', 'section'), 'split'), may hold values from -0.046875 to 0.046875
- student_input: bfloat16 [1024, 4096], P(('groups', 'split'), ('tensor', 'section')), parts along dimension 0, may hold values from -6 to 6
- student_gain: bfloat16 [4096], P(('tensor', 'section')), may hold values from 0.099609375 to 1.8984375
- gate_weight: bfloat16 [4096, 14336], P(None, ('tensor', 'section')), may hold values from -0.09375 to 0.09375
- up_weight: bfloat16 [4096, 14336], P(None, ('tensor', 'section')), may hold values from -0.09375 to 0.09375
- down_weight: bfloat16 [14336, 4096], P(('tensor', 'section')), may hold values from -0.046875 to 0.046875
- block_order: int32 [256], replicated, may hold values from 0 to 255, each once
Outputs:
- grad_gate: bfloat16 [8192, 14336], P(('groups', 'split'), ('tensor', 'section')), parts along dimension 0
- grad_up: bfloat16 [8192, 14336], P(('groups', 'split'), ('tensor', 'section')), parts along dimension 0
- grad_down: bfloat16 [28672, 4096], P(('groups', 'tensor', 'section'), 'split'), parts along dimension 0
The draws below stay inside these ranges and needn't reach their ends.
There are 2 independent parts, one for each index of `groups`. The reference program is written for one: setup_inputs(seed, part) draws one part's arguments, and reference() takes and returns one part's arrays. A program takes and returns all parts, laid end to end along the dimension named above; an argument that names none is the same for every part. Nothing has to cross between parts.
Inputs may be any that keep to these rules, and one draw needn't show every extreme that they name: `teacher_hidden`: teacher hidden states; rows differ in scale.
All inputs are finite; a program needn't handle non-finite values.
Results may differ from the reference program's by a relative error of at most 0.0083.
Values may be sent and summed in bfloat16 or wider, within the bound.
A program may use at most 256 MiB of HBM per device.

```python
import jax
import jax.numpy as jnp
from jax import lax

DT = 16384
D = 4096
FF = 14336
SHARD_ROWS = 256
TOKENS = 512
N_SECTION = 2
N_SPLIT = 2


def draw_teacher_hidden(key, part):
    first = jax.random.fold_in(key, 11)
    second = jax.random.fold_in(key, 23)
    scales = jnp.exp(jax.random.uniform(first, (TOKENS, 1), jnp.float32, 0.0, 2.302585))
    position = jnp.arange(DT, dtype=jnp.float32)[None, :] / DT
    columns = jnp.exp(position * 1.098612)
    values = jax.random.normal(second, (TOKENS, DT), jnp.float32) * scales * columns
    return jnp.clip(values, -60.0, 60.0).astype(jnp.bfloat16)


def block_scale(key, shape, cuts, smallest, high):
    factor_of, own = 1.0, jax.random.fold_in(key, 6)
    for dim, blocks in cuts:
        draws = jnp.exp(jax.random.uniform(jax.random.fold_in(own, dim), (blocks,), jnp.float32, smallest / len(cuts), high / len(cuts)))
        factor_of = factor_of * jnp.repeat(draws, shape[dim] // blocks).reshape([-1 if axis == dim else 1 for axis in range(len(shape))])
    return factor_of


def bell_draw(rng, dims, spread, bound, split=(), kind=jnp.bfloat16):
    factor_of = block_scale(rng, dims, split, -0.22, 0.18) if split else 1.0
    result = jax.random.normal(rng, dims, jnp.float32) * spread * factor_of
    return jnp.minimum(jnp.maximum(result, -bound), bound).astype(kind)


def setup_inputs(seed: int = 0, part: int = 0) -> dict:
    key_of = jax.random.split(jax.random.key(seed), 10)
    own_keys = jax.random.split(jax.random.fold_in(key_of[9], part), 10)
    teacher_hidden = draw_teacher_hidden(jax.random.fold_in(jax.random.fold_in(key_of[9], part), 71), part)
    teacher_gain = jnp.clip(1.0 + 0.18 * jax.random.normal(key_of[1], (DT,), jnp.float32), 0.1, 1.9)
    proj_weight = bell_draw(key_of[2], (DT, D), DT ** -0.5, 0.046875, ((0, 8), (1, 2)))
    student_input = bell_draw(own_keys[3], (TOKENS, D), 1.0, 6.0, ((0, 2), (1, 8)))
    student_gain = jnp.clip(1.0 + 0.18 * jax.random.normal(key_of[4], (D,), jnp.float32), 0.099609375, 1.8984375).astype(jnp.bfloat16)
    gate_weight = bell_draw(key_of[5], (D, FF), D ** -0.5, 0.09375, ((1, 8),))
    up_weight = bell_draw(key_of[6], (D, FF), D ** -0.5, 0.09375, ((1, 8),))
    down_weight = bell_draw(key_of[7], (FF, D), FF ** -0.5, 0.046875, ((0, 8),))
    block_order = jax.random.permutation(key_of[8], SHARD_ROWS).astype(jnp.int32)
    return {"teacher_hidden": teacher_hidden, "teacher_gain": teacher_gain, "proj_weight": proj_weight, "student_input": student_input, "student_gain": student_gain, "gate_weight": gate_weight, "up_weight": up_weight, "down_weight": down_weight, "block_order": block_order}


def reference(teacher_hidden, teacher_gain, proj_weight, student_input, student_gain, gate_weight, up_weight, down_weight, block_order):
    eps = 1e-05
    block = SHARD_ROWS // N_SECTION
    teach = teacher_hidden.astype(jnp.float32)
    mean_sq = lax.optimization_barrier(jnp.mean(teach * teach, axis=1, keepdims=True))
    teacher_normed = (teach * lax.rsqrt(mean_sq + eps) * teacher_gain).astype(jnp.bfloat16)
    target = jnp.dot(teacher_normed, proj_weight, preferred_element_type=jnp.float32)
    blocks = target.reshape(N_SECTION, N_SPLIT, block, D)
    per_shard = jnp.transpose(blocks, (1, 0, 2, 3)).reshape(N_SPLIT, SHARD_ROWS, D)
    arranged = jnp.take(per_shard, block_order.astype(jnp.int32), axis=1)
    matched = arranged.reshape(SHARD_ROWS * N_SPLIT, D)
    inputs = student_input.astype(jnp.float32)
    stu_sq = lax.optimization_barrier(jnp.mean(inputs * inputs, axis=1, keepdims=True))
    normed = (inputs * lax.rsqrt(stu_sq + eps) * student_gain.astype(jnp.float32)).astype(jnp.bfloat16)
    gate = jnp.dot(normed, gate_weight, preferred_element_type=jnp.float32)
    up = jnp.dot(normed, up_weight, preferred_element_type=jnp.float32)
    active = jax.nn.silu(gate)
    hidden = (active * up).astype(jnp.bfloat16)
    output = jnp.dot(hidden, down_weight, preferred_element_type=jnp.float32)
    difference = inputs + (output - matched)
    cotangent = (difference * (64.0 / (SHARD_ROWS * N_SPLIT))).astype(jnp.bfloat16)
    back_hidden = jnp.dot(cotangent, down_weight.T, preferred_element_type=jnp.float32)
    sigma = jax.nn.sigmoid(gate)
    d_gate = (back_hidden * up * sigma * (1.0 + gate * (1.0 - sigma))).astype(jnp.bfloat16)
    d_up = (back_hidden * active).astype(jnp.bfloat16)
    total_gate = jnp.zeros((D, FF), jnp.float32)
    total_up = jnp.zeros((D, FF), jnp.float32)
    total_down = jnp.zeros((FF, D), jnp.float32)
    for shard in range(N_SPLIT):
        low = shard * SHARD_ROWS
        high = low + SHARD_ROWS
        part_gate = jnp.dot(normed[low:high].T, d_gate[low:high], preferred_element_type=jnp.float32)
        part_up = jnp.dot(normed[low:high].T, d_up[low:high], preferred_element_type=jnp.float32)
        part_down = jnp.dot(hidden[low:high].T, cotangent[low:high], preferred_element_type=jnp.float32)
        total_gate = total_gate + part_gate.astype(jnp.bfloat16).astype(jnp.float32)
        total_up = total_up + part_up.astype(jnp.bfloat16).astype(jnp.float32)
        total_down = total_down + part_down.astype(jnp.bfloat16).astype(jnp.float32)
    return (total_gate.astype(jnp.bfloat16), total_up.astype(jnp.bfloat16), total_down.astype(jnp.bfloat16))
```

```python
import jax
import jax.numpy as jnp
from jax import lax
from jax.sharding import PartitionSpec as P


def swapped(value, axis):
    size = lax.axis_size(axis)
    return lax.ppermute(value, axis, [(i, i ^ 1) for i in range(size)])


def shifted(value, axis, step):
    size = lax.axis_size(axis)
    return lax.ppermute(value, axis, [(i, (i + step) % size) for i in range(size)])


def section_gathered(value):
    if lax.axis_size("section") != 2:
        return lax.all_gather(value, "section", axis=1, tiled=True)
    first = lax.axis_index("section") == 0
    other = swapped(value, "section")
    return jnp.concatenate(
        [jnp.where(first, value, other), jnp.where(first, other, value)], axis=1
    )


def section_reduced(value, after):
    if lax.axis_size("section") != 2:
        return lax.psum_scatter(value, "section", scatter_dimension=1, tiled=True)
    sec = lax.axis_index("section")
    block = value.shape[1] // 2
    away = lax.dynamic_slice_in_dim(value, (1 - sec) * block, block, 1)
    keep = lax.dynamic_slice_in_dim(value, sec * block, block, 1)
    got = swapped(away.astype(jnp.bfloat16), "section")
    if after is not None:
        got, _ = lax.optimization_barrier((got, after))
    return keep + got.astype(jnp.float32)


def gathered(piece):
    tensors = lax.axis_size("tensor")
    me = lax.axis_index("tensor")
    count = piece.shape[0]
    top = max(count // 32 * 16, 16)
    width = piece.shape[1] * lax.axis_size("section")
    steps = range(1, tensors)
    upper = [shifted(piece[:top], "tensor", step) for step in steps]
    own = section_gathered(piece)
    lower = [shifted(own[top:], "tensor", step) for step in steps]
    whole = jnp.zeros((count, width * tensors), piece.dtype)
    whole = lax.dynamic_update_slice(whole, own, (0, me * width))
    for step in steps:
        place = (me - step) % tensors * width
        pair = section_gathered(upper[step - 1])
        whole = lax.dynamic_update_slice(whole, pair, (0, place))
        whole = lax.dynamic_update_slice(whole, lower[step - 1], (top, place))
    return whole


def reduced(partial):
    tensors = lax.axis_size("tensor")
    me = lax.axis_index("tensor")
    width = partial.shape[1] // tensors
    total, last = None, None
    for step in sorted(range(tensors), key=lambda step: -min(step, tensors - step)):
        owner = (me + step) % tensors
        both = section_reduced(
            lax.dynamic_slice_in_dim(partial, owner * width, width, 1), last
        )
        if step:
            last = both.astype(jnp.bfloat16)
            both = shifted(last, "tensor", step).astype(jnp.float32)
        total = both if total is None else total + both
    return total


def summed(value):
    if lax.axis_size("section") == 2:
        value = value + swapped(value, "section")
    else:
        value = lax.psum(value, "section")
    total = value
    for step in range(1, lax.axis_size("tensor")):
        total = total + shifted(value, "tensor", step)
    return total


def on_device(
    teacher_hidden,
    teacher_gain,
    proj_weight,
    student_input,
    student_gain,
    gate_weight,
    up_weight,
    down_weight,
    block_order,
):
    eps = 1e-05
    bf16, f32 = jnp.bfloat16, jnp.float32
    sections = lax.axis_size("section")
    core = lax.axis_index("split")

    moved = lax.all_to_all(teacher_hidden, "section", split_axis=1, concat_axis=0, tiled=True)
    shard_rows = student_input.shape[0]
    gain_rows = jnp.broadcast_to(student_gain[None, :], (16, student_gain.shape[0]))
    with_gain = gathered(jnp.concatenate([student_input, gain_rows], axis=0))
    whole_input, whole_gain = with_gain[:shard_rows], with_gain[shard_rows]

    narrow = moved.shape[1]
    width = narrow * lax.axis_size("tensor") * sections
    piece_gain = lax.dynamic_slice_in_dim(
        teacher_gain, lax.axis_index("section") * narrow, narrow, 0
    )
    arranged = jnp.take(moved, block_order, axis=0)
    teach = arranged.astype(f32)
    local_sq = jnp.sum(teach * teach, axis=1)
    total_sq = summed(local_sq)
    row_scale = lax.rsqrt(total_sq / width + eps)[:, None]
    gained = (teach * piece_gain).astype(bf16)
    target_mine = jnp.dot(gained, proj_weight, preferred_element_type=f32)
    target_away = jnp.dot(swapped(gained, "split"), proj_weight, preferred_element_type=f32)
    target_got = swapped(target_away.astype(bf16), "split").astype(f32)
    target_part = row_scale * jnp.concatenate(
        [
            jnp.where(core == 0, target_mine, target_got),
            jnp.where(core == 0, target_got, target_mine),
        ],
        axis=1,
    )

    inputs = whole_input.astype(f32)
    stu_sq = jnp.mean(inputs * inputs, axis=1, keepdims=True)
    normed = (inputs * lax.rsqrt(stu_sq + eps) * whole_gain.astype(f32)).astype(bf16)
    gate = jnp.dot(normed, gate_weight, preferred_element_type=f32)
    up = jnp.dot(normed, up_weight, preferred_element_type=f32)
    active = jax.nn.silu(gate)
    hidden = (active * up).astype(bf16)
    output_part = jnp.dot(hidden, down_weight, preferred_element_type=f32)
    total_rows = shard_rows * lax.axis_size("split")
    difference = student_input.astype(f32) + reduced(output_part - target_part)
    cotangent = gathered((difference * (64.0 / total_rows)).astype(bf16))
    back_hidden = lax.dot_general(
        cotangent, down_weight, (((1,), (1,)), ((), ())), preferred_element_type=f32
    )
    sigma = jax.nn.sigmoid(gate)
    d_gate = (back_hidden * up * sigma * (1.0 + gate * (1.0 - sigma))).astype(bf16)
    d_up = (back_hidden * active).astype(bf16)

    half = normed.shape[1] // 2

    def halves(value):
        keep = lax.dynamic_slice_in_dim(value, core * half, half, 1)
        send = lax.dynamic_slice_in_dim(value, (1 - core) * half, half, 1)
        return jnp.concatenate([keep, swapped(send, "split")], axis=0)

    def rows(value):
        return jnp.concatenate([value, swapped(value, "split")], axis=0)

    def product(left, right):
        return lax.dot_general(
            left, right, (((0,), (0,)), ((), ())), preferred_element_type=f32
        ).astype(bf16)

    normed_rows = halves(normed)
    grad_down = product(rows(hidden), halves(cotangent))
    grad_gate = product(normed_rows, rows(d_gate))
    grad_up = product(normed_rows, rows(d_up))
    return grad_gate, grad_up, grad_down


def solution(mesh):
    placed = (
        P(("groups", "section", "split"), "tensor"),
        P("tensor"),
        P(("tensor", "section"), "split"),
        P(("groups", "split"), ("tensor", "section")),
        P(("tensor", "section")),
        P(None, ("tensor", "section")),
        P(None, ("tensor", "section")),
        P(("tensor", "section"), None),
        P(),
    )
    return jax.shard_map(
        on_device,
        mesh=mesh,
        in_specs=placed,
        out_specs=(
            P(("groups", "split"), ("tensor", "section")),
            P(("groups", "split"), ("tensor", "section")),
            P(("groups", "tensor", "section"), "split"),
        ),
        check_vma=False,
    )
```
